32 devices in a mesh: fsdp: 8 (over z, x), grp: 4 (over y, core).
Axes of the slice: x: 2, y: 2, z: 4, core: 2. Of those that a mesh axis runs over, the one named last changes fastest.
Arguments:
- grad: bfloat16 [28672, 8192], P('fsdp', 'grp'), may hold values from -6 to 6
- projector_t: bfloat16 [1024, 8192], P('fsdp', 'grp'), may hold values from -0.0625 to 0.0625
- first_moment: float32 [28672, 1024], P('fsdp', 'grp'), may hold values from -3 to 3
- second_moment: float32 [28672, 1024], P('fsdp', 'grp'), may hold values from 0.0001 to 0.01
Outputs:
- update: float32 [28672, 8192], P('fsdp', 'grp')
- first_new: float32 [28672, 1024], P('fsdp', 'grp')
- second_new: float32 [28672, 1024], P('fsdp', 'grp')
The draws below stay inside these ranges and needn't reach their ends.
All inputs are finite; a program needn't handle non-finite values.
Results may differ from the reference program's by a relative error of at most 0.0029.
Values may be sent and summed in bfloat16 or wider, within the bound.
A program may use at most 128 MiB of HBM per device.

```python
import math
import jax
import jax.numpy as jnp
from jax import lax

M = 8192
N = 28672
R = 1024
STEP = 10


def steps_of(own_key, extent, split, least, largest):
    level = 1.0
    for axis_at, parts in split:
        draws = jax.random.uniform(jax.random.fold_in(jax.random.fold_in(own_key, 6), axis_at), (parts,), jnp.float32, least / len(split), largest / len(split))
        level = level * jnp.repeat(jnp.exp(draws), extent[axis_at] // parts).reshape((-1,) + (1,) * (len(extent) - 1 - axis_at))
    return level


def centred(rng, dims, spread, most, cuts=(), held_as=jnp.bfloat16):
    values = spread * jax.random.normal(rng, dims, jnp.float32)
    if cuts:
        values = values * steps_of(rng, dims, cuts, -0.22, 0.18)
    return jnp.clip(values, -most, most).astype(held_as)


def setup_inputs(seed: int = 0) -> dict:
    splits = jax.random.split(jax.random.key(seed), 5)
    return {
        "grad": centred(splits[0], (N, M), 1.0, 6.0, ((0, 8), (1, 4))),
        "projector_t": centred(splits[1], (R, M), M ** -0.5, 0.0625, ((0, 8), (1, 4))),
        "first_moment": centred(splits[2], (N, R), 0.5, 3.0, ((0, 8), (1, 4)), jnp.float32),
        "second_moment": jnp.clip(jnp.exp(math.log(0.01) - 4.6051702 * jax.random.uniform(splits[3], (N, R), jnp.float32) ** steps_of(splits[3], (N, R), ((0, 8), (1, 4)), -0.2, 0.2)), 0.0001, 0.01),
    }


def reference(grad, projector_t, first_moment, second_moment):
    projected = lax.dot_general(grad, projector_t, (((1,), (1,)), ((), ())), preferred_element_type=jnp.float32)
    first_new = 0.9 * first_moment + 0.1 * projected
    second_new = 0.999 * second_moment + 0.001 * projected * projected
    correct_one = 1.0 - 0.9 ** STEP
    correct_two = 1.0 - 0.999 ** STEP
    normalized = (first_new / correct_one / (jnp.sqrt(second_new / correct_two) + 1e-08)).astype(jnp.bfloat16)
    update = jnp.dot(normalized, projector_t, preferred_element_type=jnp.float32)
    return (update, first_new, second_new)
```

```python
import jax
import jax.numpy as jnp
from jax import lax
from jax.sharding import PartitionSpec as P

STEP = 10


def flips(size):
    width = size.bit_length() - 1
    return [int(format(p, "b").zfill(width)[::-1], 2) if width else 0 for p in range(size)]


def swap(value, size, bit):
    return lax.ppermute(value, "grp", [(i, i ^ bit) for i in range(size)])


def pieces(rows):
    for count in (4, 2):
        if rows % (count * 8) == 0:
            return count
    return 1


def body(size, grad, projector_t, first_moment, second_moment):
    me = lax.axis_index("grp")
    whole = lax.all_gather(projector_t, "fsdp", axis=0, tiled=True)
    block = whole.shape[0] // size
    ranked = jnp.concatenate(
        [lax.dynamic_slice_in_dim(whole, (me ^ flip) * block, block, 0) for flip in flips(size)]
    )
    ranked = lax.optimization_barrier(ranked)
    rows = grad.shape[0]
    count = pieces(rows)
    step = rows // count
    bits = [1 << b for b in range(size.bit_length() - 1)]
    correct_one = 1.0 - 0.9**STEP
    correct_two = 1.0 - 0.999**STEP
    update = jnp.zeros((rows, grad.shape[1]), jnp.float32)
    first_new = jnp.zeros(first_moment.shape, jnp.float32)
    second_new = jnp.zeros(second_moment.shape, jnp.float32)
    for c in range(count):
        at = c * step
        part = lax.slice_in_dim(grad, at, at + step)
        half = ranked.shape[0] // 2
        total = None
        for n, bit in enumerate(bits):
            if n == 0:
                away = lax.dot_general(
                    part, ranked[half:], (((1,), (1,)), ((), ())), preferred_element_type=jnp.float32
                ).astype(jnp.bfloat16)
                total = lax.dot_general(
                    part, ranked[:half], (((1,), (1,)), ((), ())), preferred_element_type=jnp.float32
                )
            else:
                half = total.shape[1] // 2
                away = total[:, half:].astype(jnp.bfloat16)
                total = total[:, :half]
            total = total + swap(away, size, bit).astype(jnp.float32)
        one = 0.9 * first_moment[at : at + step] + 0.1 * total
        two = 0.999 * second_moment[at : at + step] + 0.001 * total * total
        full = (one / correct_one / (jnp.sqrt(two / correct_two) + 1e-08)).astype(jnp.bfloat16)
        first_new = lax.dynamic_update_slice_in_dim(first_new, one, at, 0)
        second_new = lax.dynamic_update_slice_in_dim(second_new, two, at, 0)
        for bit in reversed(bits):
            full = jnp.concatenate([full, swap(full, size, bit)], axis=1)
        out = jnp.dot(full, ranked, preferred_element_type=jnp.float32)
        update = lax.dynamic_update_slice_in_dim(update, out, at, 0)
    return (update, first_new, second_new)


def solution(mesh):
    size = mesh.shape["grp"]

    def step(*arrays):
        return body(size, *arrays)

    return jax.shard_map(
        step,
        mesh=mesh,
        in_specs=(P("fsdp", "grp"), P("fsdp", "grp"), P("fsdp", "grp"), P("fsdp", "grp")),
        out_specs=(P("fsdp", "grp"), P("fsdp", "grp"), P("fsdp", "grp")),
        check_vma=False,
    )
```
